32 devices in a mesh: grp: 8 (over y, x, core), rng: 4 (over z).
Axes of the slice: x: 2, y: 2, z: 4, core: 2. Of those that a mesh axis runs over, the one named last changes fastest.
Arguments:
- features: bfloat16 [8192, 1024], P(('grp', 'rng')), may hold values from -6 to 6
- query_weight: bfloat16 [1024, 1024], replicated
- key_weight: bfloat16 [1024, 1024], replicated
- value_weight: bfloat16 [1024, 1024], replicated, may hold values from -0.1875 to 0.1875
- out_weight: bfloat16 [1024, 1024], replicated, may hold values from -0.1875 to 0.1875
- band_reach: int32 [32], P(('grp', 'rng')), may hold values from 16 to 128, as said below
- long_peers: int32 [64, 6], P(('grp', 'rng')), may hold values from 0 to 7, as said below
- long_count: int32 [64], P(('grp', 'rng')), may hold values from 0 to 6, as said below
- send_tile: int32 [32, 8], P(('grp', 'rng')), may hold values from 0 to 3
Outputs:
- updated: bfloat16 [8192, 1024], P(('grp', 'rng'))
The draws below stay inside these ranges and needn't reach their ends.
Inputs may be any that keep to these rules, and one draw needn't show every extreme that they name: `band_reach`: some range has 128 in every draw. `long_peers`: the 6 entries of a query tile in region g are distinct regions other than g; only the first long_count entries are used. `long_count`: some query tile has 6 in every draw.
All inputs are finite; a program needn't handle non-finite values.
Results may differ from the reference program's by a relative error of at most 0.0064.
Values may be sent and summed in bfloat16 or wider, within the bound.
A program may use at most 128 MiB of HBM per device.

```python
import jax
import jax.numpy as jnp
from jax import lax

D = 1024
HEADS = 16
TOK_DEV = 256
TILE = 128
PORTAL = 64
MAXLONG = 6
REGION = 1024
NODES = 8192
QTILES = 64
N_GRP = 8
N_RNG = 4


def projection_pair(key):
    key_part = jax.random.normal(jax.random.fold_in(key, 12), (D, D), jnp.float32) * D ** (-0.5)
    query_noise = jax.random.normal(jax.random.fold_in(key, 11), (D, D), jnp.float32)
    query_part = query_noise * (D // 8) ** (-0.5)
    return (query_part, key_part)


def draw_query_weight(key, part):
    return projection_pair(key)[0].astype(jnp.bfloat16)


def draw_key_weight(key, part):
    return projection_pair(key)[1].astype(jnp.bfloat16)


def draw_band_reach(key, part):
    device_total = NODES // TOK_DEV
    reaches = jax.random.randint(jax.random.fold_in(key, 21), (device_total,), TILE // 8, TILE + 1)
    chosen = jax.random.randint(jax.random.fold_in(key, 22), (), 0, device_total)
    return jnp.where(jnp.arange(device_total) == chosen, TILE, reaches).astype(jnp.int32)


def draw_long_count(key, part):
    device_total = NODES // TOK_DEV
    per_device = TOK_DEV // TILE
    heavy_ranges = jax.random.randint(jax.random.fold_in(key, 31), (device_total,), 0, 4) == 0
    chosen = jax.random.randint(jax.random.fold_in(key, 32), (), 0, device_total)
    heavy_ranges = heavy_ranges | (jnp.arange(device_total) == chosen)
    device_cap = jnp.where(heavy_ranges, MAXLONG, MAXLONG // 3)
    tile_cap = jnp.repeat(device_cap, per_device)
    counts = jax.random.randint(jax.random.fold_in(key, 33), (QTILES,), 0, 1 << 20) % (tile_cap + 1)
    counts = jnp.where(jnp.arange(QTILES) == chosen * per_device, MAXLONG, counts)
    return counts.astype(jnp.int32)


def draw_long_peers(key, part):
    regions = NODES // REGION
    ranking_keys = jax.random.randint(jax.random.fold_in(key, 41), (QTILES, regions - 1), 0, 1 << 20) * regions
    ranking_keys = ranking_keys + jnp.arange(regions - 1, dtype=jnp.int32)[None, :]
    ranking = jnp.argsort(ranking_keys, axis=1, stable=True)[:, :MAXLONG].astype(jnp.int32)
    home_region = jnp.arange(QTILES, dtype=jnp.int32) * TILE // REGION
    return jnp.where(ranking >= home_region[:, None], ranking + 1, ranking).astype(jnp.int32)


def touch_ends(result, stream_key, least, top_value):
    spot = [jax.random.randint(jax.random.fold_in(stream_key, axis), (), 0, length) for axis, length in enumerate(result.shape)]
    main_axis = result.shape.index(max(result.shape))
    next_to = spot[:main_axis] + [(spot[main_axis] + 1) % result.shape[main_axis]] + spot[main_axis + 1:]
    return result.at[tuple(spot)].set(least).at[tuple(next_to)].set(top_value)


def block_levels(key, extent, shards, smallest, high):
    def one(dim, shards_of):
        draws = jax.random.uniform(jax.random.fold_in(jax.random.fold_in(key, 6), dim), (shards_of,), jnp.float32, smallest / len(shards), high / len(shards))
        return jnp.repeat(jnp.exp(draws), extent[dim] // shards_of).reshape((-1,) + (1,) * (len(extent) - dim - 1))

    level = one(*shards[0])
    for cut in shards[1:]:
        level = level * one(*cut)
    return level


def bell_draw(rng, dims, spread, reach, cuts=(), held_as=jnp.bfloat16):
    values = jax.random.normal(rng, dims, jnp.float32) * spread
    if len(cuts) > 0:
        values = block_levels(rng, dims, cuts, -0.22, 0.18) * values
    return jnp.clip(values, min=-reach, max=reach).astype(held_as)


def setup_inputs(seed: int = 0) -> dict:
    streams_of = jax.random.split(jax.random.key(seed), 10)
    features = bell_draw(streams_of[0], (NODES, D), 1.0, 6.0, ((0, 32),))
    query_weight = draw_query_weight(jax.random.fold_in(streams_of[9], 71), 0)
    key_weight = draw_key_weight(jax.random.fold_in(streams_of[9], 71), 0)
    value_weight = bell_draw(streams_of[3], (D, D), D ** -0.5, 0.1875)
    out_weight = bell_draw(streams_of[4], (D, D), D ** -0.5, 0.1875)
    band_reach = draw_band_reach(jax.random.fold_in(streams_of[9], 71), 0)
    long_peers = draw_long_peers(jax.random.fold_in(streams_of[9], 71), 0)
    long_count = draw_long_count(jax.random.fold_in(streams_of[9], 71), 0)
    send_tile = touch_ends(jax.random.randint(streams_of[8], (N_GRP * N_RNG, N_GRP), 0, TOK_DEV // PORTAL), jax.random.fold_in(streams_of[8], 1), 0, (TOK_DEV // PORTAL) - 1).astype(jnp.int32)
    return {"features": features, "query_weight": query_weight, "key_weight": key_weight, "value_weight": value_weight, "out_weight": out_weight, "band_reach": band_reach, "long_peers": long_peers, "long_count": long_count, "send_tile": send_tile}


EPSILON = 1e-06

def reference(features, query_weight, key_weight, value_weight, out_weight, band_reach, long_peers, long_count, send_tile):
    head_dim = D // HEADS
    score_scale = head_dim ** (-0.5)
    widened = features.astype(jnp.float32)
    normed = (widened * lax.rsqrt(lax.optimization_barrier(jnp.mean(widened * widened, axis=1, keepdims=True)) + EPSILON)).astype(jnp.bfloat16)
    queries = jnp.dot(normed, query_weight, preferred_element_type=jnp.float32).astype(jnp.bfloat16)
    keys_all = jnp.dot(normed, key_weight, preferred_element_type=jnp.float32).astype(jnp.bfloat16)
    values_all = jnp.dot(normed, value_weight, preferred_element_type=jnp.float32).astype(jnp.bfloat16)
    offsets = jnp.arange(3 * TILE, dtype=jnp.int32) - TILE
    places = jnp.arange(TILE, dtype=jnp.int32)
    inside_gap = jnp.abs(places[:, None] - offsets[None, :])
    portal_span = jnp.arange(PORTAL, dtype=jnp.int32)
    slot_ids = jnp.arange(MAXLONG, dtype=jnp.int32)

    def one_tile(tile_num):
        row_start = tile_num * TILE
        device_num = row_start // TOK_DEV
        group_num = device_num // N_RNG
        rank_num = device_num % N_RNG
        position = row_start - group_num * REGION
        band_rows = group_num * REGION + (position + offsets) % REGION
        sources = long_peers[tile_num] * N_RNG + rank_num
        portal_num = send_tile[sources, group_num]
        long_rows = (sources * TOK_DEV + portal_num * PORTAL)[:, None] + portal_span[None, :]
        key_rows = jnp.concatenate([band_rows.astype(jnp.int32), long_rows.reshape(-1).astype(jnp.int32)])
        query_blk = lax.dynamic_slice_in_dim(queries, row_start.astype(jnp.int32), TILE, 0)
        query_blk = query_blk.astype(jnp.float32).reshape(TILE, HEADS, head_dim)
        key_blk = jnp.take(keys_all, key_rows, axis=0).astype(jnp.float32).reshape(-1, HEADS, head_dim)
        value_blk = jnp.take(values_all, key_rows, axis=0).astype(jnp.float32).reshape(-1, HEADS, head_dim)
        scores = jnp.einsum('qhd,khd->hqk', query_blk, key_blk) * score_scale
        band_ok = inside_gap <= band_reach[device_num]
        long_ok = jnp.repeat(slot_ids < long_count[tile_num], PORTAL)
        allowed = jnp.concatenate([band_ok, jnp.broadcast_to(long_ok[None, :], (TILE, MAXLONG * PORTAL))], axis=1)
        scores = jnp.where(allowed[None], scores, -jnp.inf)
        highest = lax.optimization_barrier(jnp.max(scores, axis=2, keepdims=True))
        weights = jnp.exp(scores - highest)
        probabilities = (weights / lax.optimization_barrier(jnp.sum(weights, axis=2, keepdims=True))).astype(jnp.bfloat16)
        mixed = jnp.einsum('hqk,khd->qhd', probabilities.astype(jnp.float32), value_blk)
        return mixed.reshape(TILE, D).astype(jnp.bfloat16)
    attended = lax.map(one_tile, jnp.arange(QTILES, dtype=jnp.int32)).reshape(NODES, D)
    projected = jnp.dot(attended, out_weight, preferred_element_type=jnp.float32)
    return (widened + projected).astype(jnp.bfloat16)
```

```python
import functools

import jax
import jax.numpy as jnp
from jax import lax
from jax.experimental import pallas as pl
from jax.experimental.pallas import tpu as pltpu
from jax.sharding import PartitionSpec as P

HEADS = 16
TILE = 128
PORTAL = 64
EPSILON = 1e-06
LOG2E = 1.4426950408889634
VMEM_LIMIT = 48 * 1024 * 1024
MESH = pl.DeviceIdType.MESH
F32 = jnp.float32
BF16 = jnp.bfloat16


def flipped(index, offset):
    result = index
    bit = 1
    while bit <= offset:
        if offset & bit:
            result = result + bit * (1 - 2 * ((index // bit) % 2))
        bit *= 2
    return result


def rms_normed(rows):
    widened = rows.astype(F32)
    factor = lax.rsqrt(jnp.mean(widened * widened, axis=1, keepdims=True) + EPSILON)
    return (widened * factor).astype(BF16)


def nt_dot(lhs, rhs):
    return lax.dot_general(lhs, rhs, (((1,), (1,)), ((), ())), preferred_element_type=F32)


def kernel(
    n_grp,
    n_rng,
    early,
    late,
    feat_hbm,
    wq_hbm,
    wk_hbm,
    wv_hbm,
    wo_hbm,
    reach_hbm,
    peers_hbm,
    count_hbm,
    pick_hbm,
    att,
    x_ref,
    wo,
    wq,
    wk,
    wv,
    reach_ref,
    peers_ref,
    count_ref,
    pick_ref,
    stage,
    halo,
    port_e,
    port_t,
    q_s,
    xn_l,
    xn_e,
    xn_h,
    xn_t,
    acc,
    top,
    bias_l,
    bias_h,
    bias_e,
    bias_t,
    load_sem,
    small_sem,
    send_sem,
    recv_sem,
):
    rows, width = x_ref.shape
    tiles = rows // TILE
    head_dim = width // HEADS
    lanes = 2 * head_dim
    pairs = width // lanes
    grp = lax.axis_index("grp")
    rng = lax.axis_index("rng")
    loads = [
        pltpu.make_async_copy(src, dst, load_sem.at[i])
        for i, (src, dst) in enumerate(
            ((feat_hbm, x_ref), (wq_hbm, wq), (wk_hbm, wk), (wv_hbm, wv), (wo_hbm, wo))
        )
    ]
    smalls = [
        pltpu.make_async_copy(src, dst, small_sem.at[i])
        for i, (src, dst) in enumerate(
            (
                (pick_hbm, pick_ref),
                (reach_hbm, reach_ref),
                (peers_hbm, peers_ref),
                (count_hbm, count_ref),
            )
        )
    ]
    loads[0].start()
    for small in smalls:
        small.start()

    above = lax.rem(rng + 1, n_rng)
    below = lax.rem(rng + n_rng - 1, n_rng)
    barrier = pltpu.get_barrier_semaphore()
    for other in (above, below):
        pl.semaphore_signal(barrier, inc=1, device_id=(grp, other), device_id_type=MESH)
    for offset in range(1, n_grp):
        pl.semaphore_signal(
            barrier, inc=1, device_id=(flipped(grp, offset), rng), device_id_type=MESH
        )

    for load in loads[1:]:
        load.start()
    smalls[0].wait()
    loads[0].wait()
    for offset in range(1, n_grp):
        pick = jnp.full((PORTAL, width), pick_ref[0, flipped(grp, offset)], jnp.int32)
        chosen = x_ref[0:PORTAL, :]
        for i in range(1, rows // PORTAL):
            chosen = jnp.where(pick == i, x_ref[i * PORTAL : (i + 1) * PORTAL, :], chosen)
        stage[offset - 1] = chosen
    pl.semaphore_wait(barrier, n_grp + 1)

    def remote(src, dst, slot, device):
        copy = pltpu.make_async_remote_copy(
            src_ref=src,
            dst_ref=dst,
            send_sem=send_sem.at[slot],
            recv_sem=recv_sem.at[slot],
            device_id=device,
            device_id_type=MESH,
        )
        copy.start()
        return copy

    def send_portals(offsets, buffer):
        return [
            remote(
                stage.at[offset - 1],
                buffer.at[pl.ds(i * PORTAL, PORTAL)],
                1 + offset,
                (flipped(grp, offset), rng),
            )
            for i, offset in enumerate(offsets)
        ]

    early_copies = send_portals(early, port_e)
    halo_copies = [
        remote(x_ref.at[pl.ds(rows - TILE, TILE)], halo.at[0], 0, (grp, above)),
        remote(x_ref.at[pl.ds(0, TILE)], halo.at[1], 1, (grp, below)),
    ]
    late_copies = send_portals(late, port_t)
    for small in smalls[1:]:
        small.wait()

    reach = reach_ref[0]
    row_pos = lax.broadcasted_iota(jnp.int32, (rows, rows), 0)
    key_pos = lax.broadcasted_iota(jnp.int32, (rows, rows), 1)
    bias_l[...] = jnp.where(jnp.abs(row_pos - key_pos) <= reach, 0.0, -jnp.inf)
    row_pos = lax.broadcasted_iota(jnp.int32, (TILE, TILE), 0)
    key_pos = lax.broadcasted_iota(jnp.int32, (TILE, TILE), 1)
    bias_h[0] = jnp.where(row_pos + TILE - key_pos <= reach, 0.0, -jnp.inf)
    bias_h[1] = jnp.where(key_pos + TILE - row_pos <= reach, 0.0, -jnp.inf)

    def portal_bias(offsets, bias_ref):
        place = lax.broadcasted_iota(jnp.int32, (1, len(offsets) * PORTAL), 1) // PORTAL
        for t in range(tiles):
            live = jnp.zeros(place.shape, jnp.int32)
            for i, offset in enumerate(offsets):
                source = flipped(grp, offset)
                listed = jnp.int32(0)
                for s in range(peers_ref.shape[1]):
                    used = jnp.logical_and(s < count_ref[t], peers_ref[t, s] == source)
                    listed = listed + used.astype(jnp.int32)
                live = jnp.where(place == i, listed, live)
            bias_ref[t] = jnp.where(live > 0, 0.0, -jnp.inf)

    portal_bias(early, bias_e)
    portal_bias(late, bias_t)

    scale = head_dim ** (-0.5) * LOG2E
    block = 2 * lanes

    def product(weights, values):
        return jnp.dot(weights.astype(BF16), values, preferred_element_type=F32)

    def projected(source, weight, part):
        return product(source[...], weight[:, part * block : (part + 1) * block])

    def keys_of(source, part):
        return projected(source, wk, part).astype(BF16)

    def values_of(source, part):
        return projected(source, wv, part).astype(BF16)

    def split_values(values):
        low = lax.broadcasted_iota(jnp.int32, values.shape, 1) < head_dim
        one = jnp.ones_like(values)
        return jnp.where(low, values, one), jnp.where(low, one, values)

    def widened(stat, count):
        whole, rest = count // lanes, count % lanes
        parts = [stat] * whole + ([stat[:, :rest]] if rest else [])
        return jnp.concatenate(parts, axis=1) if len(parts) > 1 else parts[0]

    def q_pair(pair, places=slice(None)):
        picked = q_s[:, places, pair * lanes : (pair + 1) * lanes]
        return picked.reshape(2 * picked.shape[1], lanes)

    def spread(bias_ref, count):
        return jnp.concatenate(
            [jnp.broadcast_to(bias_ref[t], (TILE, count)) for t in range(tiles)], axis=0
        )

    def stacked(*parts):
        return jnp.concatenate([part for part in parts if part.shape[0]], axis=0)

    def local_pair(pair, keys, values):
        value_pair = split_values(values)
        both = nt_dot(q_pair(pair), keys)
        for parity in range(2):
            scores = both[parity * rows : (parity + 1) * rows] + bias_l[...]
            highest = jnp.max(scores, axis=1, keepdims=True)
            acc[pair, parity] = product(jnp.exp2(scores - highest), value_pair[parity])
            top[pair, parity] = jnp.broadcast_to(highest, (rows, lanes))

    def early_pair(pair, keys, values):
        value_pair = split_values(values)
        both = nt_dot(q_pair(pair), keys)
        for parity in range(2):
            scores = both[parity * rows : (parity + 1) * rows] + spread(bias_e, keys.shape[0])
            before = top[pair, parity]
            highest = jnp.maximum(before, jnp.max(scores, axis=1, keepdims=True))
            weights = jnp.exp2(scores - widened(highest, scores.shape[1]))
            acc[pair, parity] = acc[pair, parity] * jnp.exp2(before - highest) + product(
                weights, value_pair[parity]
            )
            top[pair, parity] = highest

    def halo_pair(pair, keys, values):
        for side in range(2):
            span = slice(side * TILE, (side + 1) * TILE)
            place = slice(side * (rows - TILE), side * (rows - TILE) + TILE)
            both = nt_dot(q_pair(pair, place), keys[span])
            value_pair = split_values(values[span])
            for parity in range(2):
                scores = both[parity * TILE : (parity + 1) * TILE] + bias_h[side]
                before = top[pair, parity, place]
                highest = jnp.maximum(before, jnp.max(scores, axis=1, keepdims=True))
                weights = jnp.exp2(scores - widened(highest, scores.shape[1]))
                acc[pair, parity, place] = acc[pair, parity, place] * jnp.exp2(
                    before - highest
                ) + product(weights, value_pair[parity])
                top[pair, parity, place] = highest

    def late_pair(pair, keys, values):
        value_pair = split_values(values)
        both = nt_dot(q_pair(pair), keys)
        halves = []
        for parity in range(2):
            scores = both[parity * rows : (parity + 1) * rows]
            scores = scores + spread(bias_t, scores.shape[1])
            before = top[pair, parity]
            highest = jnp.maximum(before, jnp.max(scores, axis=1, keepdims=True))
            weights = jnp.exp2(scores - widened(highest, scores.shape[1]))
            mixed = acc[pair, parity] * jnp.exp2(before - highest)
            halves.append(mixed + product(weights, value_pair[parity]))
        left = lax.broadcasted_iota(jnp.int32, (rows, lanes), 1) < head_dim
        even, odd = halves
        total = pltpu.roll(jnp.where(left, odd, even), head_dim, 1)
        att[:, pair * lanes : (pair + 1) * lanes] = (
            jnp.where(left, even, odd) / total
        ).astype(BF16)

    def local_queries(part):
        queries = (projected(xn_l, wq, part) * scale).astype(BF16)
        column = lax.broadcasted_iota(jnp.int32, queries.shape, 1)
        first = lax.rem(column, lanes) < head_dim
        zero = jnp.zeros_like(queries)
        cols = slice(part * block, (part + 1) * block)
        q_s[0, :, cols] = jnp.where(first, queries, zero)
        q_s[1, :, cols] = jnp.where(first, zero, queries)

    xn_l[...] = rms_normed(x_ref[...])
    loads[1].wait()
    for part in range(width // block):
        local_queries(part)
    loads[2].wait()
    loads[3].wait()

    def early_ready():
        for copy in early_copies:
            copy.wait_recv()
        xn_e[...] = rms_normed(port_e[...])

    def halo_ready():
        for copy in halo_copies:
            copy.wait_recv()
        xn_h[...] = rms_normed(halo[...].reshape(2 * TILE, width))

    def late_ready():
        for copy in late_copies:
            copy.wait_recv()
        xn_t[...] = rms_normed(port_t[...])

    steps = []
    for source, ready, attend in (
        (xn_l, None, local_pair),
        (xn_e, early_ready, early_pair),
        (xn_h, halo_ready, halo_pair),
        (xn_t, late_ready, late_pair),
    ):
        for part in range(width // block):
            steps.append((source, ready if part == 0 else None, attend, part))
    keys = keys_of(xn_l, 0)
    values = values_of(xn_l, 0)
    for number, (_, _, attend, part) in enumerate(steps):
        follower = steps[number + 1] if number + 1 < len(steps) else None
        if follower is not None and follower[1] is not None:
            follower[1]()
        attend(2 * part, keys[:, :lanes], values[:, :lanes])
        if follower is not None:
            next_keys = keys_of(follower[0], follower[3])
        attend(2 * part + 1, keys[:, lanes:], values[:, lanes:])
        if follower is not None:
            keys, values = next_keys, values_of(follower[0], follower[3])

    loads[4].wait()
    for copy in halo_copies + early_copies + late_copies:
        copy.wait_send()


def project_kernel(att_ref, x_ref, wo_ref, out_hbm, out_v, sem):
    width = out_v.shape[1]
    block = width // 4
    copies = []
    for part in range(4):
        cols = slice(part * block, (part + 1) * block)
        mixed = jnp.dot(att_ref[...], wo_ref[:, cols], preferred_element_type=F32)
        out_v[:, cols] = (x_ref[:, cols].astype(F32) + mixed).astype(BF16)
        copy = pltpu.make_async_copy(out_v.at[:, cols], out_hbm.at[:, cols], sem.at[part])
        copy.start()
        copies.append(copy)
    for copy in copies:
        copy.wait()


def local(n_grp, n_rng, features, wq, wk, wv, wo, reach, peers, count, pick):
    rows, width = features.shape
    tiles = rows // TILE
    lanes = 2 * (width // HEADS)
    pairs = width // lanes
    early = list(range(1, n_grp - 2))
    late = list(range(n_grp - 2, n_grp))
    n_early, n_late = len(early) * PORTAL, len(late) * PORTAL
    hbm = pl.BlockSpec(memory_space=pltpu.HBM)
    whole = pl.BlockSpec(memory_space=pltpu.VMEM)

    def vmem(*shape, dtype=BF16):
        return pltpu.VMEM(shape, dtype)

    def held(array):
        return pltpu.with_memory_space_constraint(array, pltpu.HBM)

    att, x, wo = pl.pallas_call(
        functools.partial(kernel, n_grp, n_rng, early, late),
        out_shape=(vmem(rows, width), vmem(rows, width), vmem(width, width)),
        in_specs=[hbm] * 9,
        out_specs=(whole,) * 3,
        scratch_shapes=[
            vmem(width, width),
            vmem(width, width),
            vmem(width, width),
            pltpu.SMEM(reach.shape, jnp.int32),
            pltpu.SMEM(peers.shape, jnp.int32),
            pltpu.SMEM(count.shape, jnp.int32),
            pltpu.SMEM(pick.shape, jnp.int32),
            vmem(n_grp - 1, PORTAL, width),
            vmem(2, TILE, width),
            vmem(n_early, width),
            vmem(n_late, width),
            vmem(2, rows, width),
            vmem(rows, width),
            vmem(n_early, width),
            vmem(2 * TILE, width),
            vmem(n_late, width),
            vmem(pairs, 2, rows, lanes, dtype=F32),
            vmem(pairs, 2, rows, lanes, dtype=F32),
            vmem(rows, rows, dtype=F32),
            vmem(2, TILE, TILE, dtype=F32),
            vmem(tiles, 1, n_early, dtype=F32),
            vmem(tiles, 1, n_late, dtype=F32),
            pltpu.SemaphoreType.DMA((5,)),
            pltpu.SemaphoreType.DMA((4,)),
            pltpu.SemaphoreType.DMA((n_grp + 1,)),
            pltpu.SemaphoreType.DMA((n_grp + 1,)),
        ],
        compiler_params=pltpu.CompilerParams(
            collective_id=0, has_side_effects=True, vmem_limit_bytes=VMEM_LIMIT
        ),
        name="graph_attention",
    )(*map(held, (features, wq, wk, wv, wo)), reach, *map(held, (peers, count, pick)))
    return pl.pallas_call(
        project_kernel,
        out_shape=jax.ShapeDtypeStruct((rows, width), BF16),
        in_specs=[whole] * 3,
        out_specs=hbm,
        scratch_shapes=[vmem(rows, width), pltpu.SemaphoreType.DMA((4,))],
        compiler_params=pltpu.CompilerParams(vmem_limit_bytes=VMEM_LIMIT // 4),
        name="out_projection",
    )(att, x, wo)


def solution(mesh):
    return jax.shard_map(
        functools.partial(local, mesh.shape["grp"], mesh.shape["rng"]),
        mesh=mesh,
        in_specs=(
            P(("grp", "rng"), None),
            P(),
            P(),
            P(),
            P(),
            P(("grp", "rng")),
            P(("grp", "rng"), None),
            P(("grp", "rng")),
            P(("grp", "rng"), None),
        ),
        out_specs=P(("grp", "rng"), None),
        check_vma=False,
    )
```

```python
import functools

import jax
import jax.numpy as jnp
from jax import lax
from jax.experimental import pallas as pl
from jax.experimental.pallas import tpu as pltpu
from jax.sharding import PartitionSpec as P

HEADS = 16
TILE = 128
PORTAL = 64
QUAD = 4
EPSILON = 1e-06
LOG2E = 1.4426950408889634
VMEM_LIMIT = 48 * 1024 * 1024
MESH = pl.DeviceIdType.MESH
F32 = jnp.float32
BF16 = jnp.bfloat16


def flipped(index, offset):
    result = index
    bit = 1
    while bit <= offset:
        if offset & bit:
            result = result + bit * (1 - 2 * ((index // bit) % 2))
        bit *= 2
    return result


def rms_normed(rows):
    widened = rows.astype(F32)
    factor = lax.rsqrt(jnp.mean(widened * widened, axis=1, keepdims=True) + EPSILON)
    return (widened * factor).astype(BF16)


def stage_plan(n_grp, rows):
    half, near = PORTAL // 2, TILE // 2
    far = near // 2
    late = (n_grp - 2, n_grp - 1)
    early = range(1, n_grp - 2)

    def portals(offsets, first, size):
        return [("portal", offset, first, size) for offset in offsets]

    def halo(distance, size):
        return [
            ("below", None, rows - distance - size, size),
            ("above", None, distance, size),
        ]

    return [
        portals([o for o in early if o == 1 or o % 2 == 0], 0, PORTAL),
        portals([o for o in early if o != 1 and o % 2 == 1], 0, PORTAL),
        halo(0, near),
        portals(late, 0, half) + halo(near, far),
        portals(late, half, half) + halo(near + far, far),
    ]


def stage_rows(blocks):
    return sum(block[3] for block in blocks)


def kernel(n_grp, n_rng, plan, *refs):
    feat_hbm, wq_hbm, wk_hbm, wv_hbm, wo_hbm, reach_hbm, peers_hbm, count_hbm, pick_hbm = refs[:9]
    att, x_ref, wo = refs[9:12]
    wq, wk, wv, reach_ref, peers_ref, count_ref, pick_ref, stage = refs[12:20]
    landed = refs[20 : 20 + len(plan)]
    biases = refs[20 + len(plan) : 21 + 2 * len(plan)]
    xn, q_t, acc, top, total, load_sem, small_sem, send_sem, recv_sem = refs[21 + 2 * len(plan) :]
    rows, width = x_ref.shape
    tiles = rows // TILE
    head_dim = width // HEADS
    block = QUAD * head_dim
    grp = lax.axis_index("grp")
    rng = lax.axis_index("rng")
    loads = [
        pltpu.make_async_copy(src, dst, load_sem.at[i])
        for i, (src, dst) in enumerate(
            ((feat_hbm, x_ref), (wq_hbm, wq), (wk_hbm, wk), (wv_hbm, wv), (wo_hbm, wo))
        )
    ]
    smalls = [
        pltpu.make_async_copy(src, dst, small_sem.at[i])
        for i, (src, dst) in enumerate(
            (
                (pick_hbm, pick_ref),
                (reach_hbm, reach_ref),
                (peers_hbm, peers_ref),
                (count_hbm, count_ref),
            )
        )
    ]
    loads[0].start()
    for small in smalls:
        small.start()

    above = lax.rem(rng + 1, n_rng)
    below = lax.rem(rng + n_rng - 1, n_rng)
    barrier = pltpu.get_barrier_semaphore()
    for other in (above, below):
        pl.semaphore_signal(barrier, inc=1, device_id=(grp, other), device_id_type=MESH)
    for offset in range(1, n_grp):
        pl.semaphore_signal(
            barrier, inc=1, device_id=(flipped(grp, offset), rng), device_id_type=MESH
        )

    for load in loads[1:]:
        load.start()
    smalls[0].wait()
    loads[0].wait()
    for offset in range(1, n_grp):
        pick = jnp.full((PORTAL, width), pick_ref[0, flipped(grp, offset)], jnp.int32)
        chosen = x_ref[0:PORTAL, :]
        for i in range(1, rows // PORTAL):
            chosen = jnp.where(pick == i, x_ref[i * PORTAL : (i + 1) * PORTAL, :], chosen)
        stage[offset - 1] = chosen
    pl.semaphore_wait(barrier, n_grp + 1)

    arrivals = []
    slot = 0
    for blocks, buffer in zip(plan, landed):
        copies = []
        place = 0
        for kind, offset, first, size in blocks:
            if kind == "portal":
                src = stage.at[offset - 1, pl.ds(first, size)]
                device = (flipped(grp, offset), rng)
            else:
                src = x_ref.at[pl.ds(first, size)]
                device = (grp, above if kind == "below" else below)
            copy = pltpu.make_async_remote_copy(
                src_ref=src,
                dst_ref=buffer.at[pl.ds(place, size)],
                send_sem=send_sem.at[slot],
                recv_sem=recv_sem.at[slot],
                device_id=device,
                device_id_type=MESH,
            )
            copy.start()
            copies.append(copy)
            place += size
            slot += 1
        arrivals.append(copies)
    for small in smalls[1:]:
        small.wait()

    reach = reach_ref[0]
    places = lax.broadcasted_iota(jnp.int32, (rows, rows), 1)
    steps = lax.broadcasted_iota(jnp.int32, (rows, rows), 0)
    biases[0][...] = jnp.where(jnp.abs(places - steps) <= reach, 0.0, -jnp.inf)
    for blocks, bias in zip(plan, biases[1:]):
        place = 0
        for kind, offset, first, size in blocks:
            span = slice(place, place + size)
            if kind == "portal":
                source = flipped(grp, offset)
                tile = lax.broadcasted_iota(jnp.int32, (size, rows), 1) // TILE
                live = jnp.zeros((size, rows), jnp.int32)
                for t in range(tiles):
                    listed = jnp.int32(0)
                    for s in range(peers_ref.shape[1]):
                        used = jnp.logical_and(s < count_ref[t], peers_ref[t, s] == source)
                        listed = listed + used.astype(jnp.int32)
                    live = jnp.where(tile == t, listed, live)
                bias[span] = jnp.where(live > 0, 0.0, -jnp.inf)
            else:
                base = first - rows if kind == "below" else first + rows
                gap = steps[:size] + base - places[:size]
                bias[span] = jnp.where(jnp.abs(gap) <= reach, 0.0, -jnp.inf)
            place += size

    scale = head_dim ** (-0.5) * LOG2E

    def projected(source, weight, part):
        return jnp.dot(
            source, weight[:, part * block : (part + 1) * block], preferred_element_type=F32
        )

    def head_only(keys, head):
        column = lax.broadcasted_iota(jnp.int32, keys.shape, 1)
        return jnp.where(column // head_dim == head, keys, jnp.zeros_like(keys))

    def scores_of(part, keys):
        count = keys.shape[0]
        lhs = jnp.concatenate([head_only(keys, head) for head in range(QUAD)], axis=0)
        queries = q_t[part * block : (part + 1) * block, :]
        stacked = jnp.dot(lhs, queries, preferred_element_type=F32)
        return [stacked[head * count : (head + 1) * count] for head in range(QUAD)]

    def weights_of(part, raw, bias, first, last):
        found = []
        for head in range(QUAD):
            number = part * QUAD + head
            scores = raw[head] + bias[...]
            highest = jnp.max(scores, axis=0, keepdims=True)
            shrink = None
            if not first:
                before = top[number : number + 1, :]
                highest = jnp.maximum(highest, before)
                shrink = jnp.exp2(before - highest)
            weights = jnp.exp2(scores - highest)
            sums = jnp.sum(weights.reshape(weights.shape[0] // 8, 8, rows), axis=0)
            if not last:
                top[number : number + 1, :] = highest
            found.append((weights.astype(BF16), sums, shrink))
        return found

    def mix(part, values, found, first, last):
        done = []
        for head in range(QUAD):
            number = part * QUAD + head
            span = slice(number * head_dim, (number + 1) * head_dim)
            weights, sums, shrink = found[head]
            mixed = jnp.dot(
                values[head * head_dim : (head + 1) * head_dim],
                weights,
                preferred_element_type=F32,
            )
            if not first:
                sums = sums + total[number] * shrink
                mixed = mixed + acc[span] * shrink
            if last:
                whole = jnp.sum(sums, axis=0, keepdims=True)
                done.append((mixed * (1.0 / whole)).astype(BF16))
            else:
                total[number] = sums
                acc[span] = mixed
        if last:
            att[:, part * block : (part + 1) * block] = jnp.concatenate(done, axis=0).T

    def run_stage(source, bias, first, last):
        parts = width // block
        keys = [projected(source[...], wk, part).astype(BF16) for part in range(parts)]

        def values_of(part):
            return projected(source[...], wv, part).astype(BF16).T

        if source.shape[0] <= TILE:
            raw = [scores_of(part, keys[part]) for part in range(parts)]
            values = [values_of(part) for part in range(parts)]
            for part in range(parts):
                found = weights_of(part, raw[part], bias, first, last)
                mix(part, values[part], found, first, last)
            return
        waiting = None
        for part in range(parts):
            raw = scores_of(part, keys[part])
            values = values_of(part)
            found = weights_of(part, raw, bias, first, last)
            if waiting is not None:
                mix(*waiting, first, last)
            waiting = (part, values, found)
        mix(*waiting, first, last)

    xn[0:rows] = rms_normed(x_ref[...])
    loads[1].wait()
    for part in range(width // block):
        queries = (projected(xn[0:rows], wq, part) * scale).astype(BF16)
        q_t[part * block : (part + 1) * block, :] = queries.T
    loads[2].wait()
    loads[3].wait()
    run_stage(xn.at[pl.ds(0, rows)], biases[0], True, False)
    place = rows
    for number, (copies, buffer) in enumerate(zip(arrivals, landed)):
        for copy in copies:
            copy.wait_recv()
        size = buffer.shape[0]
        xn[place : place + size] = rms_normed(buffer[...])
        run_stage(
            xn.at[pl.ds(place, size)], biases[number + 1], False, number + 1 == len(plan)
        )
        place += size

    loads[4].wait()
    for copies in arrivals:
        for copy in copies:
            copy.wait_send()


def project_kernel(att_ref, x_ref, wo_ref, out_hbm, out_v, sem):
    width = out_v.shape[1]
    block = width // 4
    copies = []
    for part in range(4):
        cols = slice(part * block, (part + 1) * block)
        mixed = jnp.dot(att_ref[...], wo_ref[:, cols], preferred_element_type=F32)
        out_v[:, cols] = (x_ref[:, cols].astype(F32) + mixed).astype(BF16)
        copy = pltpu.make_async_copy(out_v.at[:, cols], out_hbm.at[:, cols], sem.at[part])
        copy.start()
        copies.append(copy)
    for copy in copies:
        copy.wait()


def local(n_grp, n_rng, features, wq, wk, wv, wo, reach, peers, count, pick):
    rows, width = features.shape
    plan = stage_plan(n_grp, rows)
    sizes = [stage_rows(blocks) for blocks in plan]
    n_copies = sum(len(blocks) for blocks in plan)
    hbm = pl.BlockSpec(memory_space=pltpu.HBM)
    whole = pl.BlockSpec(memory_space=pltpu.VMEM)

    def vmem(*shape, dtype=BF16):
        return pltpu.VMEM(shape, dtype)

    def held(array):
        return pltpu.with_memory_space_constraint(array, pltpu.HBM)

    att, x, wo = pl.pallas_call(
        functools.partial(kernel, n_grp, n_rng, plan),
        out_shape=(vmem(rows, width), vmem(rows, width), vmem(width, width)),
        in_specs=[hbm] * 9,
        out_specs=(whole,) * 3,
        scratch_shapes=[
            vmem(width, width),
            vmem(width, width),
            vmem(width, width),
            pltpu.SMEM(reach.shape, jnp.int32),
            pltpu.SMEM(peers.shape, jnp.int32),
            pltpu.SMEM(count.shape, jnp.int32),
            pltpu.SMEM(pick.shape, jnp.int32),
            vmem(n_grp - 1, PORTAL, width),
            *(vmem(size, width) for size in sizes),
            *(vmem(size, rows, dtype=F32) for size in [rows] + sizes),
            vmem(rows + sum(sizes), width),
            vmem(width, rows),
            vmem(width, rows, dtype=F32),
            vmem(HEADS, rows, dtype=F32),
            vmem(HEADS, 8, rows, dtype=F32),
            pltpu.SemaphoreType.DMA((5,)),
            pltpu.SemaphoreType.DMA((4,)),
            pltpu.SemaphoreType.DMA((n_copies,)),
            pltpu.SemaphoreType.DMA((n_copies,)),
        ],
        compiler_params=pltpu.CompilerParams(
            collective_id=0, has_side_effects=True, vmem_limit_bytes=VMEM_LIMIT
        ),
        name="graph_attention",
    )(*map(held, (features, wq, wk, wv, wo)), reach, *map(held, (peers, count, pick)))
    return pl.pallas_call(
        project_kernel,
        out_shape=jax.ShapeDtypeStruct((rows, width), BF16),
        in_specs=[whole] * 3,
        out_specs=hbm,
        scratch_shapes=[vmem(rows, width), pltpu.SemaphoreType.DMA((4,))],
        compiler_params=pltpu.CompilerParams(vmem_limit_bytes=VMEM_LIMIT // 4),
        name="out_projection",
    )(att, x, wo)


def solution(mesh):
    return jax.shard_map(
        functools.partial(local, mesh.shape["grp"], mesh.shape["rng"]),
        mesh=mesh,
        in_specs=(
            P(("grp", "rng"), None),
            P(),
            P(),
            P(),
            P(),
            P(("grp", "rng")),
            P(("grp", "rng"), None),
            P(("grp", "rng")),
            P(("grp", "rng"), None),
        ),
        out_specs=P(("grp", "rng"), None),
        check_vma=False,
    )
```

```python
import functools

import jax
import jax.numpy as jnp
from jax import lax
from jax.experimental import pallas as pl
from jax.experimental.pallas import tpu as pltpu
from jax.sharding import PartitionSpec as P

HEADS = 16
TILE = 128
PORTAL = 64
QUAD = 4
EPSILON = 1e-06
LOG2E = 1.4426950408889634
VMEM_LIMIT = 48 * 1024 * 1024
MESH = pl.DeviceIdType.MESH
F32 = jnp.float32
BF16 = jnp.bfloat16


def flipped(index, offset):
    result = index
    bit = 1
    while bit <= offset:
        if offset & bit:
            result = result + bit * (1 - 2 * ((index // bit) % 2))
        bit *= 2
    return result


def rms_normed(rows):
    widened = rows.astype(F32)
    factor = lax.rsqrt(jnp.mean(widened * widened, axis=1, keepdims=True) + EPSILON)
    return (widened * factor).astype(BF16)


def stage_plan(n_grp, rows):
    half, near = PORTAL // 2, TILE // 2
    far = near // 2
    late = (n_grp - 2, n_grp - 1)
    early = range(1, n_grp - 2)

    def portals(offsets, first, size):
        return [("portal", offset, first, size) for offset in offsets]

    def halo(distance, size):
        return [
            ("below", None, rows - distance - size, size),
            ("above", None, distance, size),
        ]

    odd = [o for o in early if o > 1 and o % 2 == 1]
    return [
        portals([o for o in early if o not in odd], 0, PORTAL),
        portals(odd[:-1], 0, PORTAL) + halo(0, near)[:1],
        halo(0, near)[1:] + portals(late, 0, half),
        portals(odd[-1:], 0, PORTAL) + halo(near, far),
        portals(late, half, half) + halo(near + far, far),
    ]


def stage_rows(blocks):
    return sum(block[3] for block in blocks)


def kernel(n_grp, n_rng, plan, *refs):
    feat_hbm, wq_hbm, wk_hbm, wv_hbm, wo_hbm, reach_hbm, peers_hbm, count_hbm, pick_hbm = refs[:9]
    att, x_ref, wo = refs[9:12]
    wq, wk, wv, reach_ref, peers_ref, count_ref, pick_ref, stage = refs[12:20]
    landed = refs[20 : 20 + len(plan)]
    biases = refs[20 + len(plan) : 21 + 2 * len(plan)]
    xn, q_t, acc, top, total, load_sem, small_sem, send_sem, recv_sem, answer = refs[21 + 2 * len(plan) :]
    rows, width = x_ref.shape
    tiles = rows // TILE
    head_dim = width // HEADS
    block = QUAD * head_dim
    grp = lax.axis_index("grp")
    rng = lax.axis_index("rng")
    loads = [
        pltpu.make_async_copy(src, dst, load_sem.at[i])
        for i, (src, dst) in enumerate(
            ((feat_hbm, x_ref), (wq_hbm, wq), (wk_hbm, wk), (wv_hbm, wv), (wo_hbm, wo))
        )
    ]
    smalls = [
        pltpu.make_async_copy(src, dst, small_sem.at[i])
        for i, (src, dst) in enumerate(
            (
                (pick_hbm, pick_ref),
                (reach_hbm, reach_ref),
                (peers_hbm, peers_ref),
                (count_hbm, count_ref),
            )
        )
    ]
    loads[0].start()
    for small in smalls:
        small.start()

    above = lax.rem(rng + 1, n_rng)
    below = lax.rem(rng + n_rng - 1, n_rng)
    chip = grp // 2

    def crossed(offset):
        bits = [bit for bit in range(n_grp.bit_length()) if (offset // 2) >> bit & 1]
        held = sum((chip // (1 << bit)) % 2 for bit in bits)
        return jnp.logical_and(held > 0, held < len(bits))

    peers = []
    for offset in range(1, n_grp):
        other = flipped(grp, offset)
        apart = crossed(offset)
        straight = jnp.logical_not(apart)
        greets = jnp.logical_and(straight, grp < other)
        answers = jnp.logical_and(straight, grp > other)
        peers.append(((other, rng), greets, answers, jnp.logical_or(greets, apart), offset - 1))
    peers.append(((grp, above), rng < above, rng > above, rng < above, n_grp))
    peers.append(((grp, below), rng < below, rng > below, rng < below, n_grp - 1))
    barrier = pltpu.get_barrier_semaphore()
    greeted = jnp.int32(0)
    for device, greets, answers, _, _ in peers:

        @pl.when(greets)
        def _greet(device=device):
            pl.semaphore_signal(barrier, inc=1, device_id=device, device_id_type=MESH)

        greeted = greeted + answers.astype(jnp.int32)

    def tell(number, device):
        pl.semaphore_signal(answer.at[number], inc=1, device_id=device, device_id_type=MESH)

    def ready(number):
        @pl.when(peers[number][3])
        def _wait():
            pl.semaphore_wait(answer.at[number], 1)

    def introduce():
        for first in range(2, n_grp, 2):
            for second in range(first + 2, n_grp):
                if (first // 2) & (second // 2):
                    continue
                bits = [bit for bit in range(n_grp.bit_length()) if ((first | second) // 2) >> bit & 1]
                held = sum((chip // (1 << bit)) % 2 for bit in bits)

                @pl.when(held == 0)
                def _introduce(first=first, second=second):
                    tell((first ^ second) - 1, (flipped(grp, first), rng))
                    tell((first ^ second) - 1, (flipped(grp, second), rng))

    for load in loads[1:]:
        load.start()

    @pl.when(greeted > 0)
    def _greeted():
        pl.semaphore_wait(barrier, greeted)

    for device, _, answers, _, theirs in peers:

        @pl.when(answers)
        def _answer(device=device, theirs=theirs):
            tell(theirs, device)

    smalls[0].wait()
    loads[0].wait()
    for offset in range(1, n_grp):
        pick = jnp.full((PORTAL, width), pick_ref[0, flipped(grp, offset)], jnp.int32)
        chosen = x_ref[0:PORTAL, :]
        for i in range(1, rows // PORTAL):
            chosen = jnp.where(pick == i, x_ref[i * PORTAL : (i + 1) * PORTAL, :], chosen)
        stage[offset - 1] = chosen

    def send(kinds):
        for number, (blocks, buffer) in enumerate(zip(plan, landed)):
            place = 0
            for kind, offset, first, size in blocks:
                if kind == "portal":
                    src = stage.at[offset - 1, pl.ds(first, size)]
                    device = (flipped(grp, offset), rng)
                else:
                    src = x_ref.at[pl.ds(first, size)]
                    device = (grp, above if kind == "below" else below)
                if (kind, offset) in kinds:
                    pltpu.make_async_remote_copy(
                        src_ref=src,
                        dst_ref=buffer.at[pl.ds(place, size)],
                        send_sem=send_sem.at[0],
                        recv_sem=recv_sem.at[number],
                        device_id=device,
                        device_id_type=MESH,
                    ).start()
                place += size

    def arrived(number):
        buffer = landed[number]
        pltpu.make_async_remote_copy(
            src_ref=buffer,
            dst_ref=buffer,
            send_sem=send_sem.at[0],
            recv_sem=recv_sem.at[number],
            device_id=(grp, above),
            device_id_type=MESH,
        ).wait_recv()

    direct = list(range(1, n_grp - 2))
    for offset in [o for o in direct if o % 2 == 0] + [o for o in direct if o % 2 == 1]:
        ready(offset - 1)
        send([("portal", offset)])
    introduce()
    ready(n_grp - 1)

    @pl.when(jnp.logical_and(rng > 0, rng < n_rng - 1))
    def _send_both():
        ready(n_grp)
        send([("below", None), ("above", None)])

    @pl.when(rng == n_rng - 1)
    def _send_round_first():
        ready(n_grp)
        send([("below", None)])
        send([("above", None)])

    @pl.when(rng == 0)
    def _send_up():
        send([("below", None)])

    for small in smalls[1:]:
        small.wait()

    reach = reach_ref[0]
    places = lax.broadcasted_iota(jnp.int32, (rows, rows), 1)
    steps = lax.broadcasted_iota(jnp.int32, (rows, rows), 0)
    biases[0][...] = jnp.where(jnp.abs(places - steps) <= reach, 0.0, -jnp.inf)
    for blocks, bias in zip(plan, biases[1:]):
        place = 0
        for kind, offset, first, size in blocks:
            span = slice(place, place + size)
            if kind == "portal":
                source = flipped(grp, offset)
                tile = lax.broadcasted_iota(jnp.int32, (size, rows), 1) // TILE
                live = jnp.zeros((size, rows), jnp.int32)
                for t in range(tiles):
                    listed = jnp.int32(0)
                    for s in range(peers_ref.shape[1]):
                        used = jnp.logical_and(s < count_ref[t], peers_ref[t, s] == source)
                        listed = listed + used.astype(jnp.int32)
                    live = jnp.where(tile == t, listed, live)
                bias[span] = jnp.where(live > 0, 0.0, -jnp.inf)
            else:
                base = first - rows if kind == "below" else first + rows
                gap = steps[:size] + base - places[:size]
                bias[span] = jnp.where(jnp.abs(gap) <= reach, 0.0, -jnp.inf)
            place += size

    scale = head_dim ** (-0.5) * LOG2E

    def projected(source, weight, part):
        return jnp.dot(
            source, weight[:, part * block : (part + 1) * block], preferred_element_type=F32
        )

    def head_only(keys, head):
        column = lax.broadcasted_iota(jnp.int32, keys.shape, 1)
        return jnp.where(column // head_dim == head, keys, jnp.zeros_like(keys))

    def scores_of(part, keys):
        count = keys.shape[0]
        lhs = jnp.concatenate([head_only(keys, head) for head in range(QUAD)], axis=0)
        queries = q_t[part * block : (part + 1) * block, :]
        stacked = jnp.dot(lhs, queries, preferred_element_type=F32)
        return [stacked[head * count : (head + 1) * count] for head in range(QUAD)]

    def weights_of(part, raw, bias, first, last):
        found = []
        for head in range(QUAD):
            number = part * QUAD + head
            scores = raw[head] + bias[...]
            highest = jnp.max(scores, axis=0, keepdims=True)
            shrink = None
            if not first:
                before = top[number : number + 1, :]
                highest = jnp.maximum(highest, before)
                shrink = jnp.exp2(before - highest)
            weights = jnp.exp2(scores - highest)
            sums = jnp.sum(weights.reshape(weights.shape[0] // 8, 8, rows), axis=0)
            if not last:
                top[number : number + 1, :] = highest
            found.append((weights.astype(BF16), sums, shrink))
        return found

    def mix(part, values, found, first, last):
        done = []
        for head in range(QUAD):
            number = part * QUAD + head
            span = slice(number * head_dim, (number + 1) * head_dim)
            weights, sums, shrink = found[head]
            mixed = jnp.dot(
                values[head * head_dim : (head + 1) * head_dim],
                weights,
                preferred_element_type=F32,
            )
            if not first:
                sums = sums + total[number] * shrink
                mixed = mixed + acc[span] * shrink
            if last:
                whole = jnp.sum(sums, axis=0, keepdims=True)
                done.append((mixed * (1.0 / whole)).astype(BF16))
            else:
                total[number] = sums
                acc[span] = mixed
        if last:
            att[:, part * block : (part + 1) * block] = jnp.concatenate(done, axis=0).T

    def run_stage(source, bias, first, last):
        parts = width // block
        keys = [projected(source[...], wk, part).astype(BF16) for part in range(parts)]

        def values_of(part):
            return projected(source[...], wv, part).astype(BF16).T

        if source.shape[0] <= TILE:
            raw = [scores_of(part, keys[part]) for part in range(parts)]
            values = [values_of(part) for part in range(parts)]
            for part in range(parts):
                found = weights_of(part, raw[part], bias, first, last)
                mix(part, values[part], found, first, last)
            return
        waiting = None
        for part in range(parts):
            raw = scores_of(part, keys[part])
            values = values_of(part)
            found = weights_of(part, raw, bias, first, last)
            if waiting is not None:
                mix(*waiting, first, last)
            waiting = (part, values, found)
        mix(*waiting, first, last)

    xn[0:rows] = rms_normed(x_ref[...])
    loads[1].wait()
    for part in range(width // block):
        queries = (projected(xn[0:rows], wq, part) * scale).astype(BF16)
        q_t[part * block : (part + 1) * block, :] = queries.T
    for offset in range(n_grp - 2, n_grp):
        ready(offset - 1)
    send([("portal", offset) for offset in range(n_grp - 2, n_grp)])

    @pl.when(rng == 0)
    def _send_round():
        ready(n_grp)
        send([("above", None)])

    loads[2].wait()
    loads[3].wait()
    run_stage(xn.at[pl.ds(0, rows)], biases[0], True, False)
    place = rows
    for number, buffer in enumerate(landed):
        arrived(number)
        size = buffer.shape[0]
        xn[place : place + size] = rms_normed(buffer[...])
        run_stage(
            xn.at[pl.ds(place, size)], biases[number + 1], False, number + 1 == len(plan)
        )
        place += size

    loads[4].wait()
    sent = xn.at[pl.ds(rows, place - rows)]
    pltpu.make_async_remote_copy(
        src_ref=sent,
        dst_ref=sent,
        send_sem=send_sem.at[0],
        recv_sem=recv_sem.at[0],
        device_id=(grp, above),
        device_id_type=MESH,
    ).wait_send()


def project_kernel(att_ref, x_ref, wo_ref, out_hbm, out_v, sem):
    width = out_v.shape[1]
    block = width // 4
    copies = []
    for part in range(4):
        cols = slice(part * block, (part + 1) * block)
        mixed = jnp.dot(att_ref[...], wo_ref[:, cols], preferred_element_type=F32)
        out_v[:, cols] = (x_ref[:, cols].astype(F32) + mixed).astype(BF16)
        copy = pltpu.make_async_copy(out_v.at[:, cols], out_hbm.at[:, cols], sem.at[part])
        copy.start()
        copies.append(copy)
    for copy in copies:
        copy.wait()


def local(n_grp, n_rng, features, wq, wk, wv, wo, reach, peers, count, pick):
    rows, width = features.shape
    plan = stage_plan(n_grp, rows)
    sizes = [stage_rows(blocks) for blocks in plan]
    hbm = pl.BlockSpec(memory_space=pltpu.HBM)
    whole = pl.BlockSpec(memory_space=pltpu.VMEM)

    def vmem(*shape, dtype=BF16):
        return pltpu.VMEM(shape, dtype)

    def held(array):
        return pltpu.with_memory_space_constraint(array, pltpu.HBM)

    att, x, wo = pl.pallas_call(
        functools.partial(kernel, n_grp, n_rng, plan),
        out_shape=(vmem(rows, width), vmem(rows, width), vmem(width, width)),
        in_specs=[hbm] * 9,
        out_specs=(whole,) * 3,
        scratch_shapes=[
            vmem(width, width),
            vmem(width, width),
            vmem(width, width),
            pltpu.SMEM(reach.shape, jnp.int32),
            pltpu.SMEM(peers.shape, jnp.int32),
            pltpu.SMEM(count.shape, jnp.int32),
            pltpu.SMEM(pick.shape, jnp.int32),
            vmem(n_grp - 1, PORTAL, width),
            *(vmem(size, width) for size in sizes),
            *(vmem(size, rows, dtype=F32) for size in [rows] + sizes),
            vmem(rows + sum(sizes), width),
            vmem(width, rows),
            vmem(width, rows, dtype=F32),
            vmem(HEADS, rows, dtype=F32),
            vmem(HEADS, 8, rows, dtype=F32),
            pltpu.SemaphoreType.DMA((5,)),
            pltpu.SemaphoreType.DMA((4,)),
            pltpu.SemaphoreType.DMA((1,)),
            pltpu.SemaphoreType.DMA((len(plan),)),
            pltpu.SemaphoreType.REGULAR((n_grp + 1,)),
        ],
        compiler_params=pltpu.CompilerParams(
            collective_id=0, has_side_effects=True, vmem_limit_bytes=VMEM_LIMIT
        ),
        name="graph_attention",
    )(*map(held, (features, wq, wk, wv, wo)), reach, *map(held, (peers, count, pick)))
    return pl.pallas_call(
        project_kernel,
        out_shape=jax.ShapeDtypeStruct((rows, width), BF16),
        in_specs=[whole] * 3,
        out_specs=hbm,
        scratch_shapes=[vmem(rows, width), pltpu.SemaphoreType.DMA((4,))],
        compiler_params=pltpu.CompilerParams(vmem_limit_bytes=VMEM_LIMIT // 4),
        name="out_projection",
    )(att, x, wo)


def solution(mesh):
    return jax.shard_map(
        functools.partial(local, mesh.shape["grp"], mesh.shape["rng"]),
        mesh=mesh,
        in_specs=(
            P(("grp", "rng"), None),
            P(),
            P(),
            P(),
            P(),
            P(("grp", "rng")),
            P(("grp", "rng"), None),
            P(("grp", "rng")),
            P(("grp", "rng"), None),
        ),
        out_specs=P(("grp", "rng"), None),
        check_vma=False,
    )
```

```python
import functools

import jax
import jax.numpy as jnp
from jax import lax
from jax.experimental import pallas as pl
from jax.experimental.pallas import tpu as pltpu
from jax.sharding import PartitionSpec as P

HEADS = 16
TILE = 128
PORTAL = 64
QUAD = 4
EPSILON = 1e-06
LOG2E = 1.4426950408889634
VMEM_LIMIT = 48 * 1024 * 1024
MESH = pl.DeviceIdType.MESH
F32 = jnp.float32
BF16 = jnp.bfloat16


def flipped(index, offset):
    result = index
    bit = 1
    while bit <= offset:
        if offset & bit:
            result = result + bit * (1 - 2 * ((index // bit) % 2))
        bit *= 2
    return result


def rms_normed(rows):
    widened = rows.astype(F32)
    factor = lax.rsqrt(jnp.mean(widened * widened, axis=1, keepdims=True) + EPSILON)
    return (widened * factor).astype(BF16)


def stage_plan(n_grp, rows):
    half, near = PORTAL // 2, TILE // 2
    late = (n_grp - 2, n_grp - 1)
    early = range(1, n_grp - 2)

    def portals(offsets, first, size):
        return [("portal", offset, first, size) for offset in offsets]

    def halo(distance, size):
        return [
            ("below", None, rows - distance - size, size),
            ("above", None, distance, size),
        ]

    odd = [o for o in early if o > 1 and o % 2 == 1]
    return [
        portals([o for o in early if o not in odd], 0, PORTAL),
        portals(odd[:-1], 0, PORTAL) + halo(0, near)[:1],
        portals(odd[-1:], 0, PORTAL)
        + halo(near, near)[:1]
        + portals(late, 0, half)
        + halo(0, near)[1:],
        portals(late, half, half) + halo(near, near)[1:],
    ]


def stage_rows(blocks):
    return sum(block[3] for block in blocks)


def kernel(n_grp, n_rng, plan, *refs):
    feat_hbm, wq_hbm, wk_hbm, wv_hbm, wo_hbm, reach_hbm, peers_hbm, count_hbm, pick_hbm = refs[:9]
    att, x_ref, wo = refs[9:12]
    wq, wk, wv, reach_ref, peers_ref, count_ref, pick_ref, stage = refs[12:20]
    landed = refs[20 : 20 + len(plan)]
    biases = refs[20 + len(plan) : 21 + 2 * len(plan)]
    xn, q_t, acc, top, total, load_sem, small_sem, send_sem, recv_sem, answer = refs[21 + 2 * len(plan) :]
    rows, width = x_ref.shape
    tiles = rows // TILE
    head_dim = width // HEADS
    block = QUAD * head_dim
    grp = lax.axis_index("grp")
    rng = lax.axis_index("rng")
    loads = [
        pltpu.make_async_copy(src, dst, load_sem.at[i])
        for i, (src, dst) in enumerate(
            ((feat_hbm, x_ref), (wq_hbm, wq), (wk_hbm, wk), (wv_hbm, wv), (wo_hbm, wo))
        )
    ]
    smalls = [
        pltpu.make_async_copy(src, dst, small_sem.at[i])
        for i, (src, dst) in enumerate(
            (
                (pick_hbm, pick_ref),
                (reach_hbm, reach_ref),
                (peers_hbm, peers_ref),
                (count_hbm, count_ref),
            )
        )
    ]
    loads[0].start()
    for small in smalls:
        small.start()

    above = lax.rem(rng + 1, n_rng)
    below = lax.rem(rng + n_rng - 1, n_rng)
    chip = grp // 2

    def crossed(offset):
        bits = [bit for bit in range(n_grp.bit_length()) if (offset // 2) >> bit & 1]
        held = sum((chip // (1 << bit)) % 2 for bit in bits)
        return jnp.logical_and(held > 0, held < len(bits))

    peers = []
    for offset in range(1, n_grp):
        other = flipped(grp, offset)
        apart = crossed(offset)
        straight = jnp.logical_not(apart)
        greets = jnp.logical_and(straight, grp < other)
        answers = jnp.logical_and(straight, grp > other)
        peers.append(((other, rng), greets, answers, jnp.logical_or(greets, apart), offset - 1))
    peers.append(((grp, above), rng < above, rng > above, rng < above, n_grp))
    peers.append(((grp, below), rng < below, rng > below, rng < below, n_grp - 1))
    barrier = pltpu.get_barrier_semaphore()
    greeted = jnp.int32(0)
    for device, greets, answers, _, _ in peers:

        @pl.when(greets)
        def _greet(device=device):
            pl.semaphore_signal(barrier, inc=1, device_id=device, device_id_type=MESH)

        greeted = greeted + answers.astype(jnp.int32)

    def tell(number, device):
        pl.semaphore_signal(answer.at[number], inc=1, device_id=device, device_id_type=MESH)

    def ready(number):
        @pl.when(peers[number][3])
        def _wait():
            pl.semaphore_wait(answer.at[number], 1)

    def introduce():
        for first in range(2, n_grp, 2):
            for second in range(first + 2, n_grp):
                if (first // 2) & (second // 2):
                    continue
                bits = [bit for bit in range(n_grp.bit_length()) if ((first | second) // 2) >> bit & 1]
                held = sum((chip // (1 << bit)) % 2 for bit in bits)

                @pl.when(held == 0)
                def _introduce(first=first, second=second):
                    tell((first ^ second) - 1, (flipped(grp, first), rng))
                    tell((first ^ second) - 1, (flipped(grp, second), rng))

    for load in loads[1:]:
        load.start()

    @pl.when(greeted > 0)
    def _greeted():
        pl.semaphore_wait(barrier, greeted)

    for device, _, answers, _, theirs in peers:

        @pl.when(answers)
        def _answer(device=device, theirs=theirs):
            tell(theirs, device)

    smalls[0].wait()
    loads[0].wait()
    for offset in range(1, n_grp):
        pick = jnp.full((PORTAL, width), pick_ref[0, flipped(grp, offset)], jnp.int32)
        chosen = x_ref[0:PORTAL, :]
        for i in range(1, rows // PORTAL):
            chosen = jnp.where(pick == i, x_ref[i * PORTAL : (i + 1) * PORTAL, :], chosen)
        stage[offset - 1] = chosen

    def send(kinds):
        for number, (blocks, buffer) in enumerate(zip(plan, landed)):
            place = 0
            for kind, offset, first, size in blocks:
                if kind == "portal":
                    src = stage.at[offset - 1, pl.ds(first, size)]
                    device = (flipped(grp, offset), rng)
                else:
                    src = x_ref.at[pl.ds(first, size)]
                    device = (grp, above if kind == "below" else below)
                if (kind, offset) in kinds:
                    pltpu.make_async_remote_copy(
                        src_ref=src,
                        dst_ref=buffer.at[pl.ds(place, size)],
                        send_sem=send_sem.at[0],
                        recv_sem=recv_sem.at[number],
                        device_id=device,
                        device_id_type=MESH,
                    ).start()
                place += size

    def arrived(number):
        buffer = landed[number]
        pltpu.make_async_remote_copy(
            src_ref=buffer,
            dst_ref=buffer,
            send_sem=send_sem.at[0],
            recv_sem=recv_sem.at[number],
            device_id=(grp, above),
            device_id_type=MESH,
        ).wait_recv()

    direct = list(range(1, n_grp - 2))
    for offset in [o for o in direct if o % 2 == 0] + [o for o in direct if o % 2 == 1]:
        ready(offset - 1)
        send([("portal", offset)])
    introduce()
    ready(n_grp - 1)

    @pl.when(jnp.logical_and(rng > 0, rng < n_rng - 1))
    def _send_both():
        ready(n_grp)
        send([("below", None), ("above", None)])

    @pl.when(rng == n_rng - 1)
    def _send_round_first():
        ready(n_grp)
        send([("below", None)])
        send([("above", None)])

    @pl.when(rng == 0)
    def _send_up():
        send([("below", None)])

    for small in smalls[1:]:
        small.wait()

    reach = reach_ref[0]
    places = lax.broadcasted_iota(jnp.int32, (rows, rows), 1)
    steps = lax.broadcasted_iota(jnp.int32, (rows, rows), 0)
    biases[0][...] = jnp.where(jnp.abs(places - steps) <= reach, 0.0, -jnp.inf)
    for blocks, bias in zip(plan, biases[1:]):
        place = 0
        for kind, offset, first, size in blocks:
            span = slice(place, place + size)
            if kind == "portal":
                source = flipped(grp, offset)
                tile = lax.broadcasted_iota(jnp.int32, (size, rows), 1) // TILE
                live = jnp.zeros((size, rows), jnp.int32)
                for t in range(tiles):
                    listed = jnp.int32(0)
                    for s in range(peers_ref.shape[1]):
                        used = jnp.logical_and(s < count_ref[t], peers_ref[t, s] == source)
                        listed = listed + used.astype(jnp.int32)
                    live = jnp.where(tile == t, listed, live)
                bias[span] = jnp.where(live > 0, 0.0, -jnp.inf)
            else:
                base = first - rows if kind == "below" else first + rows
                gap = steps[:size] + base - places[:size]
                bias[span] = jnp.where(jnp.abs(gap) <= reach, 0.0, -jnp.inf)
            place += size

    scale = head_dim ** (-0.5) * LOG2E

    def projected(source, weight, part):
        return jnp.dot(
            source, weight[:, part * block : (part + 1) * block], preferred_element_type=F32
        )

    def head_only(keys, head):
        column = lax.broadcasted_iota(jnp.int32, keys.shape, 1)
        return jnp.where(column // head_dim == head, keys, jnp.zeros_like(keys))

    def scores_of(part, keys):
        count = keys.shape[0]
        lhs = jnp.concatenate([head_only(keys, head) for head in range(QUAD)], axis=0)
        queries = q_t[part * block : (part + 1) * block, :]
        stacked = jnp.dot(lhs, queries, preferred_element_type=F32)
        return [stacked[head * count : (head + 1) * count] for head in range(QUAD)]

    def weights_of(part, raw, bias, first, last):
        found = []
        for head in range(QUAD):
            number = part * QUAD + head
            scores = raw[head] + bias[...]
            highest = jnp.max(scores, axis=0, keepdims=True)
            shrink = None
            if not first:
                before = top[number : number + 1, :]
                highest = jnp.maximum(highest, before)
                shrink = jnp.exp2(before - highest)
            weights = jnp.exp2(scores - highest)
            sums = jnp.sum(weights.reshape(weights.shape[0] // 8, 8, rows), axis=0)
            if not last:
                top[number : number + 1, :] = highest
            found.append((weights.astype(BF16), sums, shrink))
        return found

    def mix(part, values, found, first, last):
        done = []
        for head in range(QUAD):
            number = part * QUAD + head
            span = slice(number * head_dim, (number + 1) * head_dim)
            weights, sums, shrink = found[head]
            mixed = jnp.dot(
                values[head * head_dim : (head + 1) * head_dim],
                weights,
                preferred_element_type=F32,
            )
            if not first:
                sums = sums + total[number] * shrink
                mixed = mixed + acc[span] * shrink
            if last:
                whole = jnp.sum(sums, axis=0, keepdims=True)
                done.append((mixed * (1.0 / whole)).astype(BF16))
            else:
                total[number] = sums
                acc[span] = mixed
        if last:
            att[:, part * block : (part + 1) * block] = jnp.concatenate(done, axis=0).T

    def run_stage(source, bias, first, last):
        parts = width // block
        keys = [projected(source[...], wk, part).astype(BF16) for part in range(parts)]

        def values_of(part):
            return projected(source[...], wv, part).astype(BF16).T

        if source.shape[0] <= TILE:
            raw = [scores_of(part, keys[part]) for part in range(parts)]
            values = [values_of(part) for part in range(parts)]
            for part in range(parts):
                found = weights_of(part, raw[part], bias, first, last)
                mix(part, values[part], found, first, last)
            return
        waiting = None
        for part in range(parts):
            raw = scores_of(part, keys[part])
            values = values_of(part)
            found = weights_of(part, raw, bias, first, last)
            if waiting is not None:
                mix(*waiting, first, last)
            waiting = (part, values, found)
        mix(*waiting, first, last)

    xn[0:rows] = rms_normed(x_ref[...])
    loads[1].wait()
    for part in range(width // block):
        queries = (projected(xn[0:rows], wq, part) * scale).astype(BF16)
        q_t[part * block : (part + 1) * block, :] = queries.T
    for offset in range(n_grp - 2, n_grp):
        ready(offset - 1)
    send([("portal", offset) for offset in range(n_grp - 2, n_grp)])

    loads[2].wait()
    loads[3].wait()
    run_stage(xn.at[pl.ds(0, rows)], biases[0], True, False)
    @pl.when(rng == 0)
    def _send_round():
        ready(n_grp)
        send([("above", None)])

    place = rows
    for number, buffer in enumerate(landed):
        arrived(number)
        size = buffer.shape[0]
        xn[place : place + size] = rms_normed(buffer[...])
        run_stage(
            xn.at[pl.ds(place, size)], biases[number + 1], False, number + 1 == len(plan)
        )
        place += size

    loads[4].wait()
    sent = xn.at[pl.ds(rows, place - rows)]
    pltpu.make_async_remote_copy(
        src_ref=sent,
        dst_ref=sent,
        send_sem=send_sem.at[0],
        recv_sem=recv_sem.at[0],
        device_id=(grp, above),
        device_id_type=MESH,
    ).wait_send()


def project_kernel(att_ref, x_ref, wo_ref, out_hbm, out_v, sem):
    width = out_v.shape[1]
    block = width // 4
    copies = []
    for part in range(4):
        cols = slice(part * block, (part + 1) * block)
        mixed = jnp.dot(att_ref[...], wo_ref[:, cols], preferred_element_type=F32)
        out_v[:, cols] = (x_ref[:, cols].astype(F32) + mixed).astype(BF16)
        copy = pltpu.make_async_copy(out_v.at[:, cols], out_hbm.at[:, cols], sem.at[part])
        copy.start()
        copies.append(copy)
    for copy in copies:
        copy.wait()


def local(n_grp, n_rng, features, wq, wk, wv, wo, reach, peers, count, pick):
    rows, width = features.shape
    plan = stage_plan(n_grp, rows)
    sizes = [stage_rows(blocks) for blocks in plan]
    hbm = pl.BlockSpec(memory_space=pltpu.HBM)
    whole = pl.BlockSpec(memory_space=pltpu.VMEM)

    def vmem(*shape, dtype=BF16):
        return pltpu.VMEM(shape, dtype)

    def held(array):
        return pltpu.with_memory_space_constraint(array, pltpu.HBM)

    att, x, wo = pl.pallas_call(
        functools.partial(kernel, n_grp, n_rng, plan),
        out_shape=(vmem(rows, width), vmem(rows, width), vmem(width, width)),
        in_specs=[hbm] * 9,
        out_specs=(whole,) * 3,
        scratch_shapes=[
            vmem(width, width),
            vmem(width, width),
            vmem(width, width),
            pltpu.SMEM(reach.shape, jnp.int32),
            pltpu.SMEM(peers.shape, jnp.int32),
            pltpu.SMEM(count.shape, jnp.int32),
            pltpu.SMEM(pick.shape, jnp.int32),
            vmem(n_grp - 1, PORTAL, width),
            *(vmem(size, width) for size in sizes),
            *(vmem(size, rows, dtype=F32) for size in [rows] + sizes),
            vmem(rows + sum(sizes), width),
            vmem(width, rows),
            vmem(width, rows, dtype=F32),
            vmem(HEADS, rows, dtype=F32),
            vmem(HEADS, 8, rows, dtype=F32),
            pltpu.SemaphoreType.DMA((5,)),
            pltpu.SemaphoreType.DMA((4,)),
            pltpu.SemaphoreType.DMA((1,)),
            pltpu.SemaphoreType.DMA((len(plan),)),
            pltpu.SemaphoreType.REGULAR((n_grp + 1,)),
        ],
        compiler_params=pltpu.CompilerParams(
            collective_id=0, has_side_effects=True, vmem_limit_bytes=VMEM_LIMIT
        ),
        name="graph_attention",
    )(*map(held, (features, wq, wk, wv, wo)), reach, *map(held, (peers, count, pick)))
    return pl.pallas_call(
        project_kernel,
        out_shape=jax.ShapeDtypeStruct((rows, width), BF16),
        in_specs=[whole] * 3,
        out_specs=hbm,
        scratch_shapes=[vmem(rows, width), pltpu.SemaphoreType.DMA((4,))],
        compiler_params=pltpu.CompilerParams(vmem_limit_bytes=VMEM_LIMIT // 4),
        name="out_projection",
    )(att, x, wo)


def solution(mesh):
    return jax.shard_map(
        functools.partial(local, mesh.shape["grp"], mesh.shape["rng"]),
        mesh=mesh,
        in_specs=(
            P(("grp", "rng"), None),
            P(),
            P(),
            P(),
            P(),
            P(("grp", "rng")),
            P(("grp", "rng"), None),
            P(("grp", "rng")),
            P(("grp", "rng"), None),
        ),
        out_specs=P(("grp", "rng"), None),
        check_vma=False,
    )
```

```python
import functools

import jax
import jax.numpy as jnp
from jax import lax
from jax.experimental import pallas as pl
from jax.experimental.pallas import tpu as pltpu
from jax.sharding import PartitionSpec as P

HEADS = 16
TILE = 128
PORTAL = 64
QUAD = 4
EPSILON = 1e-06
LOG2E = 1.4426950408889634
VMEM_LIMIT = 48 * 1024 * 1024
MESH = pl.DeviceIdType.MESH
F32 = jnp.float32
BF16 = jnp.bfloat16


def flipped(index, offset):
    result = index
    bit = 1
    while bit <= offset:
        if offset & bit:
            result = result + bit * (1 - 2 * ((index // bit) % 2))
        bit *= 2
    return result


def rms_normed(rows):
    widened = rows.astype(F32)
    factor = lax.rsqrt(jnp.mean(widened * widened, axis=1, keepdims=True) + EPSILON)
    return (widened * factor).astype(BF16)


def stage_plan(n_grp, rows):
    half, near = PORTAL // 2, TILE // 2
    late = (n_grp - 2, n_grp - 1)
    early = range(1, n_grp - 2)

    def portals(offsets, first, size):
        return [("portal", offset, first, size) for offset in offsets]

    def halo(distance, size):
        return [
            ("below", None, rows - distance - size, size),
            ("above", None, distance, size),
        ]

    odd = [o for o in early if o > 1 and o % 2 == 1]
    return [
        portals([o for o in early if o not in odd], 0, PORTAL),
        portals(odd[:-1], 0, PORTAL) + halo(0, near)[:1],
        portals(odd[-1:], 0, PORTAL)
        + halo(near, near)[:1]
        + portals(late, 0, half)
        + halo(0, near)[1:],
        portals(late, half, half) + halo(near, near)[1:],
    ]


def stage_rows(blocks):
    return sum(block[3] for block in blocks)


def kernel(n_grp, n_rng, plan, *refs):
    feat_hbm, wq_hbm, wk_hbm, wv_hbm, wo_hbm, reach_hbm, peers_hbm, count_hbm, pick_hbm = refs[:9]
    att, x_ref, wo = refs[9:12]
    wq, wk, wv, reach_ref, peers_ref, count_ref, pick_ref, stage = refs[12:20]
    landed = refs[20 : 20 + len(plan)]
    biases = refs[20 + len(plan) : 21 + 2 * len(plan)]
    xn, q_t, acc, top, total, load_sem, small_sem, send_sem, recv_sem, answer = refs[21 + 2 * len(plan) :]
    rows, width = x_ref.shape
    tiles = rows // TILE
    head_dim = width // HEADS
    block = QUAD * head_dim
    grp = lax.axis_index("grp")
    rng = lax.axis_index("rng")
    loads = [
        pltpu.make_async_copy(src, dst, load_sem.at[i])
        for i, (src, dst) in enumerate(
            ((feat_hbm, x_ref), (wq_hbm, wq), (wk_hbm, wk), (wv_hbm, wv), (wo_hbm, wo))
        )
    ]
    smalls = [
        pltpu.make_async_copy(src, dst, small_sem.at[i])
        for i, (src, dst) in enumerate(
            (
                (pick_hbm, pick_ref),
                (reach_hbm, reach_ref),
                (peers_hbm, peers_ref),
                (count_hbm, count_ref),
            )
        )
    ]
    loads[0].start()
    for small in smalls:
        small.start()

    above = lax.rem(rng + 1, n_rng)
    below = lax.rem(rng + n_rng - 1, n_rng)
    chip = grp // 2

    def crossed(offset):
        bits = [bit for bit in range(n_grp.bit_length()) if (offset // 2) >> bit & 1]
        held = sum((chip // (1 << bit)) % 2 for bit in bits)
        return jnp.logical_and(held > 0, held < len(bits))

    peers = []
    for offset in range(1, n_grp):
        other = flipped(grp, offset)
        apart = crossed(offset)
        straight = jnp.logical_not(apart)
        greets = jnp.logical_and(straight, grp < other)
        answers = jnp.logical_and(straight, grp > other)
        peers.append(((other, rng), greets, answers, jnp.logical_or(greets, apart), offset - 1))
    peers.append(((grp, above), rng < above, rng > above, rng < above, n_grp))
    peers.append(((grp, below), rng < below, rng > below, rng < below, n_grp - 1))
    barrier = pltpu.get_barrier_semaphore()
    greeted = jnp.int32(0)
    for device, greets, answers, _, _ in peers:

        @pl.when(greets)
        def _greet(device=device):
            pl.semaphore_signal(barrier, inc=1, device_id=device, device_id_type=MESH)

        greeted = greeted + answers.astype(jnp.int32)

    def tell(number, device):
        pl.semaphore_signal(answer.at[number], inc=1, device_id=device, device_id_type=MESH)

    def ready(number):
        @pl.when(peers[number][3])
        def _wait():
            pl.semaphore_wait(answer.at[number], 1)

    def introduce():
        for first in range(2, n_grp, 2):
            for second in range(first + 2, n_grp):
                if (first // 2) & (second // 2):
                    continue
                bits = [bit for bit in range(n_grp.bit_length()) if ((first | second) // 2) >> bit & 1]
                held = sum((chip // (1 << bit)) % 2 for bit in bits)

                @pl.when(held == 0)
                def _introduce(first=first, second=second):
                    tell((first ^ second) - 1, (flipped(grp, first), rng))
                    tell((first ^ second) - 1, (flipped(grp, second), rng))

    for load in loads[1:]:
        load.start()

    @pl.when(greeted > 0)
    def _greeted():
        pl.semaphore_wait(barrier, greeted)

    for device, _, answers, _, theirs in peers:

        @pl.when(answers)
        def _answer(device=device, theirs=theirs):
            tell(theirs, device)

    smalls[0].wait()
    loads[0].wait()
    for offset in range(1, n_grp):
        pick = jnp.full((PORTAL, width), pick_ref[0, flipped(grp, offset)], jnp.int32)
        chosen = x_ref[0:PORTAL, :]
        for i in range(1, rows // PORTAL):
            chosen = jnp.where(pick == i, x_ref[i * PORTAL : (i + 1) * PORTAL, :], chosen)
        stage[offset - 1] = chosen

    def send(kinds):
        for number, (blocks, buffer) in enumerate(zip(plan, landed)):
            place = 0
            for kind, offset, first, size in blocks:
                if kind == "portal":
                    src = stage.at[offset - 1, pl.ds(first, size)]
                    device = (flipped(grp, offset), rng)
                else:
                    src = x_ref.at[pl.ds(first, size)]
                    device = (grp, above if kind == "below" else below)
                if (kind, offset) in kinds:
                    pltpu.make_async_remote_copy(
                        src_ref=src,
                        dst_ref=buffer.at[pl.ds(place, size)],
                        send_sem=send_sem.at[0],
                        recv_sem=recv_sem.at[number],
                        device_id=device,
                        device_id_type=MESH,
                    ).start()
                place += size

    def arrived(number):
        buffer = landed[number]
        pltpu.make_async_remote_copy(
            src_ref=buffer,
            dst_ref=buffer,
            send_sem=send_sem.at[0],
            recv_sem=recv_sem.at[number],
            device_id=(grp, above),
            device_id_type=MESH,
        ).wait_recv()

    direct = list(range(1, n_grp - 2))
    for offset in [o for o in direct if o % 2 == 0] + [o for o in direct if o % 2 == 1]:
        ready(offset - 1)
        send([("portal", offset)])
    introduce()
    ready(n_grp - 1)

    @pl.when(jnp.logical_and(rng > 0, rng < n_rng - 1))
    def _send_both():
        ready(n_grp)
        send([("below", None), ("above", None)])

    @pl.when(rng == n_rng - 1)
    def _send_round_first():
        ready(n_grp)
        send([("below", None)])
        send([("above", None)])

    @pl.when(rng == 0)
    def _send_up():
        send([("below", None)])

    for small in smalls[1:]:
        small.wait()

    reach = reach_ref[0]
    places = lax.broadcasted_iota(jnp.int32, (rows, rows), 1)
    steps = lax.broadcasted_iota(jnp.int32, (rows, rows), 0)
    biases[0][...] = jnp.where(jnp.abs(places - steps) <= reach, 0.0, -jnp.inf)
    for blocks, bias in zip(plan, biases[1:]):
        place = 0
        for kind, offset, first, size in blocks:
            span = slice(place, place + size)
            if kind == "portal":
                source = flipped(grp, offset)
                tile = lax.broadcasted_iota(jnp.int32, (size, rows), 1) // TILE
                live = jnp.zeros((size, rows), jnp.int32)
                for t in range(tiles):
                    listed = jnp.int32(0)
                    for s in range(peers_ref.shape[1]):
                        used = jnp.logical_and(s < count_ref[t], peers_ref[t, s] == source)
                        listed = listed + used.astype(jnp.int32)
                    live = jnp.where(tile == t, listed, live)
                bias[span] = jnp.where(live > 0, 0.0, -jnp.inf)
            else:
                base = first - rows if kind == "below" else first + rows
                gap = steps[:size] + base - places[:size]
                bias[span] = jnp.where(jnp.abs(gap) <= reach, 0.0, -jnp.inf)
            place += size

    scale = head_dim ** (-0.5) * LOG2E

    def projected(source, weight, part):
        return jnp.dot(
            source, weight[:, part * block : (part + 1) * block], preferred_element_type=F32
        )

    def head_only(keys, head):
        column = lax.broadcasted_iota(jnp.int32, keys.shape, 1)
        return jnp.where(column // head_dim == head, keys, jnp.zeros_like(keys))

    def scores_of(part, keys):
        count = keys.shape[0]
        lhs = jnp.concatenate([head_only(keys, head) for head in range(QUAD)], axis=0)
        queries = q_t[part * block : (part + 1) * block, :]
        stacked = jnp.dot(lhs, queries, preferred_element_type=F32)
        return [stacked[head * count : (head + 1) * count] for head in range(QUAD)]

    def weights_of(part, raw, bias, first, last):
        found = []
        for head in range(QUAD):
            number = part * QUAD + head
            scores = raw[head] + bias[...]
            highest = jnp.max(scores, axis=0, keepdims=True)
            shrink = None
            if not first:
                before = top[number : number + 1, :]
                highest = jnp.maximum(highest, before)
                shrink = jnp.exp2(before - highest)
            weights = jnp.exp2(scores - highest)
            sums = jnp.sum(weights.reshape(weights.shape[0] // 8, 8, rows), axis=0)
            if not last:
                top[number : number + 1, :] = highest
            found.append((weights.astype(BF16), sums, shrink))
        return found

    def mix(part, values, found, first, last):
        done = []
        for head in range(QUAD):
            number = part * QUAD + head
            span = slice(number * head_dim, (number + 1) * head_dim)
            weights, sums, shrink = found[head]
            mixed = jnp.dot(
                values[head * head_dim : (head + 1) * head_dim],
                weights,
                preferred_element_type=F32,
            )
            if not first:
                sums = sums + total[number] * shrink
                mixed = mixed + acc[span] * shrink
            if last:
                whole = jnp.sum(sums, axis=0, keepdims=True)
                done.append((mixed * (1.0 / whole)).astype(BF16))
            else:
                total[number] = sums
                acc[span] = mixed
        if last:
            att[:, part * block : (part + 1) * block] = jnp.concatenate(done, axis=0).T

    def run_stage(source, bias, first, last):
        parts = width // block
        keys = [projected(source[...], wk, part).astype(BF16) for part in range(parts)]

        def values_of(part):
            return projected(source[...], wv, part).astype(BF16).T

        if source.shape[0] <= TILE:
            raw = [scores_of(part, keys[part]) for part in range(parts)]
            values = [values_of(part) for part in range(parts)]
            for part in range(parts):
                found = weights_of(part, raw[part], bias, first, last)
                mix(part, values[part], found, first, last)
            return
        waiting = None
        for part in range(parts):
            raw = scores_of(part, keys[part])
            values = values_of(part)
            found = weights_of(part, raw, bias, first, last)
            if waiting is not None:
                mix(*waiting, first, last)
            waiting = (part, values, found)
        mix(*waiting, first, last)

    xn[0:rows] = rms_normed(x_ref[...])
    loads[1].wait()
    for part in range(width // block):
        queries = (projected(xn[0:rows], wq, part) * scale).astype(BF16)
        q_t[part * block : (part + 1) * block, :] = queries.T
    for offset in range(n_grp - 2, n_grp):
        ready(offset - 1)
    send([("portal", offset) for offset in range(n_grp - 2, n_grp)])

    loads[2].wait()
    loads[3].wait()
    run_stage(xn.at[pl.ds(0, rows)], biases[0], True, False)
    @pl.when(rng == 0)
    def _send_round():
        ready(n_grp)
        send([("above", None)])

    place = rows
    for number, buffer in enumerate(landed):
        arrived(number)
        size = buffer.shape[0]
        xn[place : place + size] = rms_normed(buffer[...])
        run_stage(
            xn.at[pl.ds(place, size)], biases[number + 1], False, number + 1 == len(plan)
        )
        place += size

    loads[4].wait()
    sent = xn.at[pl.ds(rows, place - rows)]
    pltpu.make_async_remote_copy(
        src_ref=sent,
        dst_ref=sent,
        send_sem=send_sem.at[0],
        recv_sem=recv_sem.at[0],
        device_id=(grp, above),
        device_id_type=MESH,
    ).wait_send()


def project_kernel(att_ref, x_ref, wo_ref, out_hbm, out_v, sem):
    width = out_v.shape[1]
    block = width // 2
    for part in range(2):
        cols = slice(part * block, (part + 1) * block)
        mixed = jnp.dot(att_ref[...], wo_ref[:, cols], preferred_element_type=F32)
        out_v[:, cols] = (x_ref[:, cols].astype(F32) + mixed).astype(BF16)
        pltpu.make_async_copy(out_v.at[:, cols], out_hbm.at[:, cols], sem.at[0]).start()
    pltpu.make_async_copy(out_v, out_hbm, sem.at[0]).wait()


def local(n_grp, n_rng, features, wq, wk, wv, wo, reach, peers, count, pick):
    rows, width = features.shape
    plan = stage_plan(n_grp, rows)
    sizes = [stage_rows(blocks) for blocks in plan]
    hbm = pl.BlockSpec(memory_space=pltpu.HBM)
    whole = pl.BlockSpec(memory_space=pltpu.VMEM)

    def vmem(*shape, dtype=BF16):
        return pltpu.VMEM(shape, dtype)

    def held(array):
        return pltpu.with_memory_space_constraint(array, pltpu.HBM)

    att, x, wo = pl.pallas_call(
        functools.partial(kernel, n_grp, n_rng, plan),
        out_shape=(vmem(rows, width), vmem(rows, width), vmem(width, width)),
        in_specs=[hbm] * 9,
        out_specs=(whole,) * 3,
        scratch_shapes=[
            vmem(width, width),
            vmem(width, width),
            vmem(width, width),
            pltpu.SMEM(reach.shape, jnp.int32),
            pltpu.SMEM(peers.shape, jnp.int32),
            pltpu.SMEM(count.shape, jnp.int32),
            pltpu.SMEM(pick.shape, jnp.int32),
            vmem(n_grp - 1, PORTAL, width),
            *(vmem(size, width) for size in sizes),
            *(vmem(size, rows, dtype=F32) for size in [rows] + sizes),
            vmem(rows + sum(sizes), width),
            vmem(width, rows),
            vmem(width, rows, dtype=F32),
            vmem(HEADS, rows, dtype=F32),
            vmem(HEADS, 8, rows, dtype=F32),
            pltpu.SemaphoreType.DMA((5,)),
            pltpu.SemaphoreType.DMA((4,)),
            pltpu.SemaphoreType.DMA((1,)),
            pltpu.SemaphoreType.DMA((len(plan),)),
            pltpu.SemaphoreType.REGULAR((n_grp + 1,)),
        ],
        compiler_params=pltpu.CompilerParams(
            collective_id=0, has_side_effects=True, vmem_limit_bytes=VMEM_LIMIT
        ),
        name="graph_attention",
    )(*map(held, (features, wq, wk, wv, wo)), reach, *map(held, (peers, count, pick)))
    return pl.pallas_call(
        project_kernel,
        out_shape=jax.ShapeDtypeStruct((rows, width), BF16),
        in_specs=[whole] * 3,
        out_specs=hbm,
        scratch_shapes=[vmem(rows, width), pltpu.SemaphoreType.DMA((1,))],
        compiler_params=pltpu.CompilerParams(vmem_limit_bytes=VMEM_LIMIT // 4),
        name="out_projection",
    )(att, x, wo)


def solution(mesh):
    return jax.shard_map(
        functools.partial(local, mesh.shape["grp"], mesh.shape["rng"]),
        mesh=mesh,
        in_specs=(
            P(("grp", "rng"), None),
            P(),
            P(),
            P(),
            P(),
            P(("grp", "rng")),
            P(("grp", "rng"), None),
            P(("grp", "rng")),
            P(("grp", "rng"), None),
        ),
        out_specs=P(("grp", "rng"), None),
        check_vma=False,
    )
```
